16 devices in a mesh: dp: 4 (over y, z, core), tp: 4 (over x).
Axes of the slice: x: 4, y: 2, z: 1, core: 2. Of those that a mesh axis runs over, the one named last changes fastest.
The devices are a block of a 4x4x8 slice.
Arguments:
- x: bfloat16 [4096, 6656], P(('dp', 'tp')), parts along dimension 0
- gain: bfloat16 [6656], replicated
- wq: bfloat16 [6656, 6656], P(None, 'tp')
- wk: bfloat16 [6656, 6656], P(None, 'tp')
- wv: bfloat16 [6656, 6656], P(None, 'tp')
- wo: bfloat16 [6656, 6656], P('tp')
Outputs:
- output: bfloat16 [4096, 6656], P(('dp', 'tp')), parts along dimension 0
There are 4 independent parts. The reference program is written for one: setup_inputs(seed, part) draws one part's arguments, and reference() takes and returns one part's arrays. A program takes and returns all parts, laid end to end along the dimension named above; an argument that names none is the same for every part.
All inputs are finite; a program needn't handle non-finite values.
Results may differ from the reference program's by a relative error of at most 0.012.
Values are sent between devices in bfloat16 or wider.
A program may use at most 768 MiB of HBM per device.

```python
import jax
import jax.numpy as jnp
from jax import lax

ROWS = 1024
D = 6656
HEADS = 52
KV_HEADS = 52
HEAD = 128
THETA = 10000


def setup_inputs(seed: int = 0, part: int = 0) -> dict:
    kx, kn, kq, kk, kv, ko = jax.random.split(jax.random.key(seed), 6)

    def weights(key, rows, columns):
        return jax.random.normal(key, (rows, columns), jnp.float32) * rows**-0.5

    drawn = {
        "x": jax.random.normal(jax.random.fold_in(kx, part), (ROWS, D), jnp.float32),
        "gain": 1 + 0.1 * jax.random.normal(kn, (D,), jnp.float32),
        "wq": 2 * weights(kq, D, HEADS * HEAD),
        "wk": 2 * weights(kk, D, KV_HEADS * HEAD),
        "wv": 4 * weights(kv, D, KV_HEADS * HEAD),
        "wo": weights(ko, HEADS * HEAD, D),
    }
    return {k: v.astype(jnp.bfloat16) for k, v in drawn.items()}


def normed(x, gain):
    wide = x.astype(jnp.float32)
    scale = lax.rsqrt(jnp.mean(wide * wide, -1, keepdims=True) + 1e-6)
    return (wide * scale * gain.astype(jnp.float32)).astype(jnp.bfloat16)


def turned(t, place, theta):
    half = t.shape[-1] // 2
    angle = place.astype(jnp.float32)[:, None] * theta ** (-jnp.arange(half, dtype=jnp.float32) / half)
    cos, sin = jnp.cos(angle)[:, None], jnp.sin(angle)[:, None]
    a, b = t[..., :half].astype(jnp.float32), t[..., half:].astype(jnp.float32)
    return jnp.concatenate([a * cos - b * sin, b * cos + a * sin], -1).astype(jnp.bfloat16)


def matmul(a, w):
    return jnp.dot(a, w, preferred_element_type=jnp.float32).astype(jnp.bfloat16)


def einsum(form, a, b):
    return jnp.einsum(form, a.astype(jnp.float32), b.astype(jnp.float32))


def attention(q, k, v):
    scores = einsum("tgsd,ugd->gstu", q, k) * q.shape[-1] ** -0.5
    token = jnp.arange(q.shape[0])
    scores = jnp.where(token[:, None] >= token, scores, -jnp.inf)
    weights = jax.nn.softmax(scores, -1).astype(jnp.bfloat16)
    return einsum("gstu,ugd->tgsd", weights, v).astype(jnp.bfloat16)


def reference(x, gain, wq, wk, wv, wo):
    a, place = normed(x, gain), jnp.arange(ROWS)
    q = turned(matmul(a, wq).reshape(ROWS, HEADS, HEAD), place, THETA).reshape(ROWS, KV_HEADS, -1, HEAD)
    k = turned(matmul(a, wk).reshape(ROWS, KV_HEADS, HEAD), place, THETA)
    v = matmul(a, wv).reshape(ROWS, KV_HEADS, HEAD)
    seen = attention(q, k, v).reshape(ROWS, HEADS * HEAD)
    return (x.astype(jnp.float32) + jnp.dot(seen, wo, preferred_element_type=jnp.float32)).astype(jnp.bfloat16)
```

```python
import functools

import jax
import jax.numpy as jnp
import numpy as np
from jax import lax
from jax.experimental import pallas as pl
from jax.experimental.pallas import tpu as pltpu
from jax.sharding import PartitionSpec as P

HEAD = 128
THETA = 10000
KC = 512
UC = KC // HEAD
AHEAD = 2
SLOTS = 3
NEG = -1e30
HIDDEN = 2 * NEG
LOG2E = 1.4426950408889634
BF, F32 = jnp.bfloat16, jnp.float32
MESH = pl.DeviceIdType.MESH


def _dot(a, b, ca, cb):
    return lax.dot_general(a, b, (((ca,), (cb,)), ((), ())), preferred_element_type=F32)


def _kernel(x_ref, gain_ref, freq_ref, wq_ref, wk_ref, wv_ref, wo_ref, y_ref, xg, acc, wbuf, cos_s, sin_s, top_s,
            s_opp, s_full, r_half, r_full, ag_send, ag_recv, rs_send, rs_recv, w_sem, wo_sem, x_sem, y_sem):
    R, D = x_ref.shape
    n_tp = xg.shape[1] // R
    T = n_tp * R
    U = D // HEAD
    NC = D // KC
    HK = wo_ref.shape[0]
    H = HK // HEAD
    R2 = R // 2
    me = lax.axis_index("tp")
    right, left = lax.rem(me + 1, n_tp), lax.rem(me + n_tp - 1, n_tp)
    opp = lax.rem(me + 2, n_tp)

    def rows(b, start=0, size=R):
        return pl.ds(pl.multiple_of(b * R + start, R2), size)

    weights = (wq_ref, wk_ref, wv_ref)

    def w_copy(c, i):
        return pltpu.make_async_copy(
            weights[i].at[pl.ds(pl.multiple_of(c * KC, KC), KC), :],
            wbuf.at[lax.rem(c, 2), :, i * HK : (i + 1) * HK],
            w_sem.at[lax.rem(c, 2), i])

    pieces = [(k, min(KC, HK - k)) for k in range(0, HK, KC)]
    width = len(pieces) * KC
    first_slot = (NC - 2) % 2

    def wo_place(s):
        place = lax.rem(s, 4)
        return place, lax.rem(first_slot + lax.div(place, 2), 2), lax.rem(place, 2) * width

    def wo_copy(s, i):
        place, slot, off = wo_place(s)
        k, size = pieces[i]
        n = lax.rem(s, NC)
        return pltpu.make_async_copy(
            wo_ref.at[k : k + size, pl.ds(pl.multiple_of(n * KC, KC), KC)],
            wbuf.at[slot, 0:size, pl.ds(pl.multiple_of(off + i * KC, KC), KC)],
            wo_sem.at[place, i])

    def wo_start(s):
        for i in range(len(pieces)):
            wo_copy(s, i).start()

    def wo_wait(s):
        for i in range(len(pieces)):
            wo_copy(s, i).wait()

    def wo_cols(s, at, size):
        _, slot, off = wo_place(s)
        return jnp.concatenate(
            [wbuf[slot, 0:ks, pl.ds(pl.multiple_of(off + i * KC + at, HEAD), size)] for i, (k, ks) in enumerate(pieces)], axis=0)

    def seen(b):
        return jnp.concatenate([xg[3 * H + h, rows(b), :] for h in range(H)], axis=1)

    def ag_rows(kind, came):
        if kind == 0:
            return rows(left if came else me)
        if kind == 1:
            return rows(right if came else me)
        if kind == 2:
            return rows(opp if came else left, 0, R2)
        return rows(opp if came else right, R2, R2)

    def ag(kind, c, came=False):
        ref = xg.at[pl.ds(c * UC, UC), ag_rows(kind, came), :]
        return pltpu.make_async_remote_copy(ref, ref, ag_send.at[kind, c], ag_recv.at[kind, c],
                                            device_id={"tp": left if kind % 2 else right}, device_id_type=MESH)

    def rs(kind, n):
        if kind < 2:
            src, dst = s_opp.at[n, kind * R2 : (kind + 1) * R2, :], r_half.at[kind, n]
        else:
            src, dst = s_full.at[kind - 2, lax.rem(n, SLOTS)], r_full.at[kind - 2, n]
        return pltpu.make_async_remote_copy(src, dst, rs_send.at[kind, n], rs_recv.at[kind, n],
                                            device_id={"tp": left if kind % 2 else right}, device_id_type=MESH)

    def x_copy(u):
        return pltpu.make_async_copy(x_ref.at[:, pl.ds(pl.multiple_of(u * HEAD, HEAD), HEAD)], xg.at[u, rows(me), :], x_sem.at[0])

    lax.fori_loop(0, U, lambda u, _: x_copy(u).start(), None)
    for c in range(2):
        for i in range(3):
            w_copy(c, i).start()
    barrier = pltpu.get_barrier_semaphore()
    for other in (left, right):
        pl.semaphore_signal(barrier, inc=1, device_id={"tp": other}, device_id_type=MESH)
    own = xg.at[:, rows(me), :]
    pltpu.make_async_copy(own, own, x_sem.at[0]).wait()

    group = 32

    def sums(g, _):
        here = pl.ds(pl.multiple_of(me * R + g * group, group), group)

        def add(u, s):
            t = xg[u, here, :].astype(F32)
            return s + t * t

        s = lax.fori_loop(0, U, add, jnp.zeros((group, HEAD), F32), unroll=4)
        scale = lax.rsqrt(s.sum(-1, keepdims=True) / D + 1e-6)
        acc[0, pl.ds(pl.multiple_of(g * group, group), group), :] = jnp.broadcast_to(scale, (group, HEAD))

    lax.fori_loop(0, R // group, sums, None)
    pl.semaphore_wait(barrier, 2)

    def norm(c, _):
        def unit(j, _):
            u = c * UC + j
            xg[u, rows(me), :] = (xg[u, rows(me), :].astype(F32) * acc[0, :R, :] * gain_ref[u]).astype(BF)

        lax.fori_loop(0, UC, unit, None)

        @pl.when(c <= AHEAD)
        def _():
            ag(0, c).start()
            ag(1, c).start()

    lax.fori_loop(0, NC, norm, None)

    step = 128

    def angles(g, _):
        here = pl.ds(pl.multiple_of(g * step, step), step)
        place = (lax.broadcasted_iota(jnp.int32, (step, HEAD), 0) + g * step).astype(F32)
        angle = place * freq_ref[...]
        lane = lax.broadcasted_iota(jnp.int32, (step, HEAD), 1)
        sin = jnp.sin(angle)
        cos_s[here, :] = jnp.cos(angle)
        sin_s[here, :] = jnp.where(lane < HEAD // 2, -sin, sin)

    lax.fori_loop(0, T // step, angles, None)

    def clear(u, _):
        acc[u] = jnp.zeros((T, HEAD), F32)

    lax.fori_loop(0, 3 * H, clear, None)

    def product(c, at, size):
        lhs = jnp.concatenate([xg[c * UC + j] for j in range(UC)], axis=1)
        return jnp.dot(lhs, wbuf[lax.rem(c, 2), :, pl.ds(pl.multiple_of(at, HEAD), size)], preferred_element_type=F32)

    def add_pair(c, i, count=2):
        r = product(c, i * 2 * HEAD, count * HEAD)
        for j in range(count):
            acc[2 * i + j] += r[:, j * HEAD : (j + 1) * HEAD]

    def end_pair(c, i, turn, count=2):
        r = product(c, i * 2 * HEAD, count * HEAD)
        for j in range(count):
            t = (acc[2 * i + j] + r[:, j * HEAD : (j + 1) * HEAD]).astype(BF)
            if turn:
                t = t.astype(F32)
                t = (t * cos_s[...] + pltpu.roll(t, HEAD // 2, 1) * sin_s[...]).astype(BF)
            xg[2 * i + j] = t

    pairs, odd = 3 * H // 2, 3 * H % 2

    def multiply(c):
        for i in range(3):
            w_copy(c, i).wait()
        lax.fori_loop(0, pairs, lambda i, _: add_pair(c, i), None)
        if odd:
            add_pair(c, pairs, 1)

    def gather(c, _):
        ag(0, c, True).wait_recv()
        ag(1, c, True).wait_recv()
        ag(2, c).start()
        ag(3, c).start()

        @pl.when(c + AHEAD + 1 < NC)
        def _():
            ag(0, c + AHEAD + 1).start()
            ag(1, c + AHEAD + 1).start()

        @pl.when(c >= 1)
        def _():
            ag(2, c - 1, True).wait_recv()
            ag(3, c - 1, True).wait_recv()
            multiply(c - 1)

            @pl.when(c + 1 < NC)
            def _():
                for i in range(3):
                    w_copy(c + 1, i).start()

    lax.fori_loop(0, NC, gather, None)
    wo_start(0)
    wo_start(1)

    def sent(c, _):
        for kind in range(4):
            ag(kind, c).wait_send()

    lax.fori_loop(0, NC, sent, None)
    ag(2, NC - 1, True).wait_recv()
    ag(3, NC - 1, True).wait_recv()
    for i in range(3):
        w_copy(NC - 1, i).wait()
    lax.fori_loop(0, H, lambda i, _: end_pair(NC - 1, i, True), None)
    lax.fori_loop(H, pairs, lambda i, _: end_pair(NC - 1, i, False), None)
    if odd:
        end_pair(NC - 1, pairs, False, 1)
    wo_start(2)
    wo_start(3)

    e = HEAD**-0.5 * LOG2E
    ones = jnp.ones((8, R), BF)

    tall = HEAD + 8
    parts = [(q, q // HEAD * 2 * HEAD) for q in range(0, R, HEAD)]

    def mix(h):
        return jnp.concatenate([acc[h, at : at + tall, :] for _, at in parts], axis=1)

    def attend(b):
        for h in range(H):
            top_s[h : h + 1, :] = jnp.full((1, R), NEG, F32)
            for _, at in parts:
                acc[h, at : at + tall, :] = jnp.zeros((tall, HEAD), F32)

        def block(j, masked):
            scores = [_dot(xg[H + h, rows(j), :], xg[h, rows(b), :], 1, 1) for h in range(H)]
            weights, keeps = [], []
            for h, s in enumerate(scores):
                if masked:
                    ok = lax.broadcasted_iota(jnp.int32, (R, R), 1) >= lax.broadcasted_iota(jnp.int32, (R, R), 0)
                    s = jnp.where(ok, s, HIDDEN)
                old = top_s[h : h + 1, :]
                top = jnp.maximum(old, s.max(axis=0, keepdims=True))
                top_s[h : h + 1, :] = top
                weights.append(jnp.exp2((s - top) * e).astype(BF))
                keeps.append(jnp.exp2((old - top) * e))
            for h, (p, keep) in enumerate(zip(weights, keeps)):
                values = jnp.concatenate([xg[2 * H + h, rows(j), :].T, ones], axis=0)
                new = mix(h) * keep + _dot(values, p, 1, 0)
                for q, at in parts:
                    acc[h, at : at + tall, :] = new[:, q : q + HEAD]

        lax.fori_loop(0, b, lambda j, _: block(j, False), None)
        block(b, True)
        for h in range(H):
            got = mix(h)
            xg[3 * H + h, rows(b), :] = (got[:HEAD] * (1 / got[HEAD : HEAD + 1])).T.astype(BF)

    half = KC // 2

    def send_opp(n, _):
        wo_wait(n)
        for at in (0, half):
            s_opp[n, :, at : at + half] = jnp.dot(seen(opp), wo_cols(n, at, half), preferred_element_type=F32).astype(BF)
        rs(0, n).start()
        rs(1, n).start()
        wo_start(n + 4)

    def attention(i, _):
        b = jnp.where(i == 0, opp, jnp.where(i == 1, right, jnp.where(i == 2, left, me)))
        attend(b)

        @pl.when(i == 0)
        def _():
            lax.fori_loop(0, NC, send_opp, None)

    lax.fori_loop(0, n_tp, attention, None)

    def tile_copy(n, j, out):
        hbm = (y_ref if out else x_ref).at[:, pl.ds(pl.multiple_of(n * KC + j * HEAD, HEAD), HEAD)]
        vmem = xg.at[n if out else H + n, rows(j), :]
        return pltpu.make_async_copy(vmem, hbm, y_sem.at[n]) if out else pltpu.make_async_copy(hbm, vmem, x_sem.at[n])

    def x_start(n, _):
        for j in range(UC):
            tile_copy(n, j, False).start()

    lax.fori_loop(0, NC, x_start, None)

    def send_full(n):
        wo_wait(n + NC)
        rs(0, n).wait_recv()
        rs(1, n).wait_recv()

        @pl.when(n >= SLOTS)
        def _():
            rs(2, n - SLOTS).wait_send()
            rs(3, n - SLOTS).wait_send()

        slot = lax.rem(n, SLOTS)
        lhs = jnp.concatenate([seen(right), seen(left), seen(me)], axis=0)
        for at in (0, half):
            cols = slice(at, at + half)
            r = jnp.dot(lhs, wo_cols(n + NC, at, half), preferred_element_type=F32)
            s_full[0, slot, :R2, cols] = (r[:R2] + r_half[0, n, :, cols].astype(F32)).astype(BF)
            s_full[0, slot, R2:, cols] = r[R2:R].astype(BF)
            s_full[1, slot, :R2, cols] = r[R : R + R2].astype(BF)
            s_full[1, slot, R2:, cols] = (r[R + R2 : 2 * R] + r_half[1, n, :, cols].astype(F32)).astype(BF)
            for j in range(half // HEAD):
                acc[n, rows(at // HEAD + j), :] = r[2 * R :, j * HEAD : (j + 1) * HEAD]
        rs(2, n).start()
        rs(3, n).start()

        @pl.when(n + 4 < NC)
        def _():
            wo_start(n + NC + 4)

    def finish(n):
        rs(2, n).wait_recv()
        rs(3, n).wait_recv()
        tile = xg.at[H + n]
        pltpu.make_async_copy(tile, tile, x_sem.at[n]).wait()
        for j in range(UC):
            cols = slice(j * HEAD, (j + 1) * HEAD)
            total = acc[n, rows(j), :] + r_full[0, n, :, cols].astype(F32) + r_full[1, n, :, cols].astype(F32)
            xg[n, rows(j), :] = (xg[H + n, rows(j), :].astype(F32) + total).astype(BF)
        for j in range(UC):
            tile_copy(n, j, True).start()

    def both(n, _):
        @pl.when(n < NC)
        def _():
            send_full(n)

        @pl.when(n >= SLOTS)
        def _():
            finish(n - SLOTS)

    lax.fori_loop(0, NC + SLOTS, both, None)

    def end(n, _):
        rs(0, n).wait_send()
        rs(1, n).wait_send()

        @pl.when(n >= NC - SLOTS)
        def _():
            rs(2, n).wait_send()
            rs(3, n).wait_send()

        tile = xg.at[n]
        pltpu.make_async_copy(tile, tile, y_sem.at[n]).wait()

    lax.fori_loop(0, NC, end, None)


def layer(x, gain, wq, wk, wv, wo, n_tp):
    R, D = x.shape
    HK = wo.shape[0]
    H = HK // HEAD
    T, U, NC = n_tp * R, D // HEAD, D // KC
    half = HEAD // 2
    freq = np.tile(np.float32(THETA) ** (-np.arange(half, dtype=np.float32) / np.float32(half)), 2)[None]
    any_, vmem = pl.BlockSpec(memory_space=pl.ANY), pl.BlockSpec(memory_space=pltpu.VMEM)
    dma = pltpu.SemaphoreType.DMA
    return pl.pallas_call(
        _kernel,
        out_shape=jax.ShapeDtypeStruct((R, D), BF),
        in_specs=[any_, vmem, vmem, any_, any_, any_, any_],
        out_specs=any_,
        scratch_shapes=[
            pltpu.VMEM((U, T, HEAD), BF),
            pltpu.VMEM((3 * H, T, HEAD), F32),
            pltpu.VMEM((2, KC, 3 * HK), BF),
            pltpu.VMEM((T, HEAD), F32),
            pltpu.VMEM((T, HEAD), F32),
            pltpu.VMEM((H, R), F32),
            pltpu.VMEM((NC, R, KC), BF),
            pltpu.VMEM((2, SLOTS, R, KC), BF),
            pltpu.VMEM((2, NC, R // 2, KC), BF),
            pltpu.VMEM((2, NC, R, KC), BF),
            dma((4, NC)), dma((4, NC)), dma((4, NC)), dma((4, NC)),
            dma((2, 3)), dma((4, -(-HK // KC))), dma((NC,)), dma((NC,)),
        ],
        compiler_params=pltpu.CompilerParams(collective_id=0, has_side_effects=True, vmem_limit_bytes=67043328),
        cost_estimate=pl.CostEstimate(flops=8 * T * D * HK, bytes_accessed=8 * D * HK, transcendentals=H * T * T),
    )(x, gain.astype(F32).reshape(U, 1, HEAD), jnp.asarray(freq), wq, wk, wv, wo)


def solution(mesh):
    tokens, columns = P(("dp", "tp"), None), P(None, "tp")
    return jax.shard_map(
        functools.partial(layer, n_tp=mesh.shape["tp"]),
        mesh=mesh,
        in_specs=(tokens, P(None), columns, columns, columns, P("tp", None)),
        out_specs=tokens,
        check_vma=False,
    )
```

```python
import functools

import jax
import jax.numpy as jnp
import numpy as np
from jax import lax
from jax.experimental import pallas as pl
from jax.experimental.pallas import tpu as pltpu
from jax.sharding import PartitionSpec as P

HEAD = 128
THETA = 10000
KC = 512
UC = KC // HEAD
AHEAD = 1
SLOTS = 2
NEG = -1e30
HIDDEN = 2 * NEG
LOG2E = 1.4426950408889634
BF, F32 = jnp.bfloat16, jnp.float32
MESH = pl.DeviceIdType.MESH


def _dot(a, b, ca, cb):
    return lax.dot_general(a, b, (((ca,), (cb,)), ((), ())), preferred_element_type=F32)


def _kernel(x_ref, gain_ref, freq_ref, wq_ref, wk_ref, wv_ref, wo_ref, y_ref, xg, acc, wbuf, cos_s, sin_s, top_s,
            s_opp, s_full, r_half, r_full, ag_send, ag_recv, rs_send, rs_recv, w_sem, wo_sem, x_sem, y_sem):
    R, D = x_ref.shape
    n_tp = xg.shape[1] // R
    T = n_tp * R
    U = D // HEAD
    NC = D // KC
    HK = wo_ref.shape[0]
    H = HK // HEAD
    R2 = R // 2
    me = lax.axis_index("tp")
    right, left = lax.rem(me + 1, n_tp), lax.rem(me + n_tp - 1, n_tp)

    OWN, RIGHT, LEFT, OPP = range(4)

    def rows(place, start=0, size=R):
        at = place * R + start
        return pl.ds(at if isinstance(place, int) else pl.multiple_of(at, R2), size)

    def swap(i):
        return jnp.where(i == 2, 3, jnp.where(i == 3, 2, i))

    weights = (wq_ref, wk_ref, wv_ref)

    def w_copy(c, i):
        return pltpu.make_async_copy(
            weights[i].at[pl.ds(pl.multiple_of(c * KC, KC), KC), :],
            wbuf.at[lax.rem(c, 2), :, i * HK : (i + 1) * HK],
            w_sem.at[lax.rem(c, 2), i])

    pieces = [(k, min(KC, HK - k)) for k in range(0, HK, KC)]
    width = len(pieces) * KC
    first_slot = (NC - 2) % 2

    def wo_place(s):
        place = lax.rem(s, 4)
        return place, lax.rem(first_slot + lax.div(place, 2), 2), lax.rem(place, 2) * width

    def wo_copy(s, i):
        place, slot, off = wo_place(s)
        k, size = pieces[i]
        n = lax.rem(s, NC)
        return pltpu.make_async_copy(
            wo_ref.at[k : k + size, pl.ds(pl.multiple_of(n * KC, KC), KC)],
            wbuf.at[slot, 0:size, pl.ds(pl.multiple_of(off + i * KC, KC), KC)],
            wo_sem.at[place, i])

    def wo_start(s):
        for i in range(len(pieces)):
            wo_copy(s, i).start()

    def wo_wait(s):
        for i in range(len(pieces)):
            wo_copy(s, i).wait()

    def wo_cols(s, at, size):
        _, slot, off = wo_place(s)
        return jnp.concatenate(
            [wbuf[slot, 0:ks, pl.ds(pl.multiple_of(off + i * KC + at, HEAD), size)] for i, (k, ks) in enumerate(pieces)], axis=0)

    def seen(here):
        return jnp.concatenate([xg[3 * H + h, here, :] for h in range(H)], axis=1)

    def ag_rows(kind, came):
        if kind == 0:
            return rows(LEFT if came else OWN)
        if kind == 1:
            return rows(RIGHT if came else OWN)
        if kind == 2:
            return rows(OPP if came else LEFT, 0, R2)
        return rows(OPP if came else RIGHT, R2, R2)

    def ag(kind, c):
        src = xg.at[pl.ds(c * UC, UC), ag_rows(kind, False), :]
        dst = xg.at[pl.ds(c * UC, UC), ag_rows(kind, True), :]
        return pltpu.make_async_remote_copy(src, dst, ag_send.at[kind, c], ag_recv.at[kind, c],
                                            device_id={"tp": left if kind % 2 else right}, device_id_type=MESH)

    def rs(kind, n):
        if kind < 2:
            src, dst = s_opp.at[n, kind * R2 : (kind + 1) * R2, :], r_half.at[kind, n]
        else:
            src, dst = s_full.at[kind - 2, lax.rem(n, SLOTS)], r_full.at[kind - 2, n]
        return pltpu.make_async_remote_copy(src, dst, rs_send.at[kind, n], rs_recv.at[kind, n],
                                            device_id={"tp": left if kind % 2 else right}, device_id_type=MESH)

    def x_copy(u):
        return pltpu.make_async_copy(x_ref.at[:, pl.ds(pl.multiple_of(u * HEAD, HEAD), HEAD)], xg.at[u, rows(OWN), :], x_sem.at[0])

    lax.fori_loop(0, U, lambda u, _: x_copy(u).start(), None)
    for c in range(2):
        for i in range(3):
            w_copy(c, i).start()
    barrier = pltpu.get_barrier_semaphore()
    for other in (left, right):
        pl.semaphore_signal(barrier, inc=1, device_id={"tp": other}, device_id_type=MESH)
    own = xg.at[:, rows(OWN), :]
    pltpu.make_async_copy(own, own, x_sem.at[0]).wait()

    group = 32

    def sums(g, _):
        here = pl.ds(pl.multiple_of(g * group, group), group)

        def add(u, s):
            t = xg[u, here, :].astype(F32)
            return s + t * t

        s = lax.fori_loop(0, U, add, jnp.zeros((group, HEAD), F32), unroll=4)
        scale = lax.rsqrt(s.sum(-1, keepdims=True) / D + 1e-6)
        acc[0, pl.ds(pl.multiple_of(g * group, group), group), :] = jnp.broadcast_to(scale, (group, HEAD))

    lax.fori_loop(0, R // group, sums, None)
    pl.semaphore_wait(barrier, 2)

    def norm(c, _):
        def unit(j, _):
            u = c * UC + j
            xg[u, rows(OWN), :] = (xg[u, rows(OWN), :].astype(F32) * acc[0, :R, :] * gain_ref[u]).astype(BF)

        lax.fori_loop(0, UC, unit, None)

        @pl.when(c <= AHEAD)
        def _():
            ag(0, c).start()
            ag(1, c).start()

    lax.fori_loop(0, NC, norm, None)

    step = 128

    def angles(g, _):
        here = pl.ds(pl.multiple_of(g * step, step), step)
        at = g * step
        first = lax.rem(me + swap(lax.div(at, R)), n_tp) * R + lax.rem(at, R)
        place = (lax.broadcasted_iota(jnp.int32, (step, HEAD), 0) + first).astype(F32)
        angle = place * freq_ref[...]
        lane = lax.broadcasted_iota(jnp.int32, (step, HEAD), 1)
        sin = jnp.sin(angle)
        cos_s[here, :] = jnp.cos(angle)
        sin_s[here, :] = jnp.where(lane < HEAD // 2, -sin, sin)

    lax.fori_loop(0, T // step, angles, None)

    def clear(u, _):
        acc[u] = jnp.zeros((T, HEAD), F32)

    lax.fori_loop(0, 3 * H, clear, None)

    early, late = slice(0, 3 * R), slice(3 * R, 4 * R)
    wide = 4
    tiles = [(u, min(wide, 3 * H - u)) for u in range(0, 3 * H, wide)]

    def product(chunks, here, u, count):
        lhs = jnp.concatenate([xg[c * UC + j, here, :] for c in chunks for j in range(UC)], axis=1)
        rhs = jnp.concatenate([wbuf[lax.rem(c, 2), :, u * HEAD : (u + count) * HEAD] for c in chunks], axis=0)
        return jnp.dot(lhs, rhs, preferred_element_type=F32)

    def multiply(c, here):
        for u, count in tiles:
            r = product([c], here, u, count)
            for j in range(count):
                acc[u + j, here, :] += r[:, j * HEAD : (j + 1) * HEAD]

    def end(chunks, here):
        for u, count in tiles:
            r = product(chunks, here, u, count)
            for j in range(count):
                t = (acc[u + j, here, :] + r[:, j * HEAD : (j + 1) * HEAD]).astype(BF)
                if u + j < 2 * H:
                    t = t.astype(F32)
                    t = (t * cos_s[here, :] + pltpu.roll(t, HEAD // 2, 1) * sin_s[here, :]).astype(BF)
                xg[u + j, here, :] = t

    def near(c):
        ag(0, c).wait_recv()
        ag(1, c).wait_recv()
        ag(2, c).start()
        ag(3, c).start()

    def far(c):
        ag(2, c).wait_recv()
        ag(3, c).wait_recv()

    def w_wait(c):
        for i in range(3):
            w_copy(c, i).wait()

    def gather(c, _):
        near(c)

        @pl.when(c + AHEAD + 1 < NC)
        def _():
            ag(0, c + AHEAD + 1).start()
            ag(1, c + AHEAD + 1).start()

        w_wait(c)
        multiply(c, early)

        @pl.when(c >= 1)
        def _():
            far(c - 1)
            multiply(c - 1, late)
            for i in range(3):
                w_copy(c + 1, i).start()

    lax.fori_loop(0, NC - 1, gather, None)
    near(NC - 1)
    held = -(-3 * H // UC)

    def sent(c, _):
        for kind in range(4):
            ag(kind, c).wait_send()

    lax.fori_loop(0, held, sent, None)
    w_wait(NC - 1)
    end([NC - 1], early)
    far(NC - 2)
    far(NC - 1)
    end([NC - 2, NC - 1], late)
    lax.fori_loop(held, NC, sent, None)
    for i in range(4):
        wo_start(i)

    e = HEAD**-0.5 * LOG2E
    ones = jnp.ones((8, R), BF)

    tall = HEAD + 8
    parts = [(q, q // HEAD * 2 * HEAD) for q in range(0, R, HEAD)]

    def mix(h):
        return jnp.concatenate([acc[h, at : at + tall, :] for _, at in parts], axis=1)

    def attend(b, at_q):
        for h in range(H):
            top_s[h : h + 1, :] = jnp.full((1, R), NEG, F32)
            for _, at in parts:
                acc[h, at : at + tall, :] = jnp.zeros((tall, HEAD), F32)

        def block(j, masked):
            keys = rows(swap(lax.rem(j - me + n_tp, n_tp)))
            scores = [_dot(xg[H + h, keys, :], xg[h, at_q, :], 1, 1) for h in range(H)]
            weights, keeps = [], []
            for h, s in enumerate(scores):
                if masked:
                    ok = lax.broadcasted_iota(jnp.int32, (R, R), 1) >= lax.broadcasted_iota(jnp.int32, (R, R), 0)
                    s = jnp.where(ok, s, HIDDEN)
                old = top_s[h : h + 1, :]
                top = jnp.maximum(old, s.max(axis=0, keepdims=True))
                top_s[h : h + 1, :] = top
                weights.append(jnp.exp2((s - top) * e).astype(BF))
                keeps.append(jnp.exp2((old - top) * e))
            for h, (p, keep) in enumerate(zip(weights, keeps)):
                values = jnp.concatenate([xg[2 * H + h, keys, :].T, ones], axis=0)
                new = mix(h) * keep + _dot(values, p, 1, 0)
                for q, at in parts:
                    acc[h, at : at + tall, :] = new[:, q : q + HEAD]

        lax.fori_loop(0, b, lambda j, _: block(j, False), None)
        block(b, True)
        for h in range(H):
            got = mix(h)
            xg[3 * H + h, at_q, :] = (got[:HEAD] * (1 / got[HEAD : HEAD + 1])).T.astype(BF)

    half = KC // 2

    def send_opp(n, _):
        wo_wait(n)
        for at in (0, half):
            s_opp[n, :, at : at + half] = jnp.dot(seen(late), wo_cols(n, at, half), preferred_element_type=F32).astype(BF)
        rs(0, n).start()
        rs(1, n).start()
        wo_start(n + 4)

    def attention(i, _):
        place = jnp.where(i == 0, OPP, jnp.where(i == 3, OWN, i))
        attend(lax.rem(me + swap(place), n_tp), rows(place))

        @pl.when(i == 0)
        def _():
            lax.fori_loop(0, NC, send_opp, None)

    lax.fori_loop(0, n_tp, attention, None)

    def tile_copy(n, j, out):
        hbm = (y_ref if out else x_ref).at[:, pl.ds(pl.multiple_of(n * KC + j * HEAD, HEAD), HEAD)]
        vmem = xg.at[n if out else H + n, rows(j), :]
        return pltpu.make_async_copy(vmem, hbm, y_sem.at[n]) if out else pltpu.make_async_copy(hbm, vmem, x_sem.at[n])

    def x_start(n, _):
        for j in range(UC):
            tile_copy(n, j, False).start()

    lax.fori_loop(0, NC, x_start, None)

    def send_full(n):
        wo_wait(n + NC)
        rs(0, n).wait_recv()
        rs(1, n).wait_recv()

        @pl.when(n >= SLOTS)
        def _():
            rs(2, n - SLOTS).wait_send()
            rs(3, n - SLOTS).wait_send()

        slot = lax.rem(n, SLOTS)
        lhs = seen(early)
        for at in (0, half):
            cols = slice(at, at + half)
            r = jnp.dot(lhs, wo_cols(n + NC, at, half), preferred_element_type=F32)
            own, to_right, to_left = r[:R], r[R : 2 * R], r[2 * R :]
            s_full[0, slot, :R2, cols] = (to_right[:R2] + r_half[0, n, :, cols].astype(F32)).astype(BF)
            s_full[0, slot, R2:, cols] = to_right[R2:].astype(BF)
            s_full[1, slot, :R2, cols] = to_left[:R2].astype(BF)
            s_full[1, slot, R2:, cols] = (to_left[R2:] + r_half[1, n, :, cols].astype(F32)).astype(BF)
            for j in range(half // HEAD):
                acc[n, rows(at // HEAD + j), :] = own[:, j * HEAD : (j + 1) * HEAD]
        rs(2, n).start()
        rs(3, n).start()

        @pl.when(n + 4 < NC)
        def _():
            wo_start(n + NC + 4)

    def finish(n):
        rs(2, n).wait_recv()
        rs(3, n).wait_recv()
        tile = xg.at[H + n]
        pltpu.make_async_copy(tile, tile, x_sem.at[n]).wait()
        for j in range(UC):
            cols = slice(j * HEAD, (j + 1) * HEAD)
            total = acc[n, rows(j), :] + r_full[0, n, :, cols].astype(F32) + r_full[1, n, :, cols].astype(F32)
            xg[n, rows(j), :] = (xg[H + n, rows(j), :].astype(F32) + total).astype(BF)
        for j in range(UC):
            tile_copy(n, j, True).start()

    def both(n, _):
        @pl.when(n < NC)
        def _():
            send_full(n)

        @pl.when(n >= SLOTS)
        def _():
            finish(n - SLOTS)

    lax.fori_loop(0, NC + SLOTS, both, None)

    def close(n, _):
        rs(0, n).wait_send()
        rs(1, n).wait_send()

        @pl.when(n >= NC - SLOTS)
        def _():
            rs(2, n).wait_send()
            rs(3, n).wait_send()

        tile = xg.at[n]
        pltpu.make_async_copy(tile, tile, y_sem.at[n]).wait()

    lax.fori_loop(0, NC, close, None)


def layer(x, gain, wq, wk, wv, wo, n_tp):
    R, D = x.shape
    HK = wo.shape[0]
    H = HK // HEAD
    T, U, NC = n_tp * R, D // HEAD, D // KC
    half = HEAD // 2
    freq = np.tile(np.float32(THETA) ** (-np.arange(half, dtype=np.float32) / np.float32(half)), 2)[None]
    any_, vmem = pl.BlockSpec(memory_space=pl.ANY), pl.BlockSpec(memory_space=pltpu.VMEM)
    dma = pltpu.SemaphoreType.DMA
    return pl.pallas_call(
        _kernel,
        out_shape=jax.ShapeDtypeStruct((R, D), BF),
        in_specs=[any_, vmem, vmem, any_, any_, any_, any_],
        out_specs=any_,
        scratch_shapes=[
            pltpu.VMEM((U, T, HEAD), BF),
            pltpu.VMEM((3 * H, T, HEAD), F32),
            pltpu.VMEM((2, KC, 3 * HK), BF),
            pltpu.VMEM((T, HEAD), F32),
            pltpu.VMEM((T, HEAD), F32),
            pltpu.VMEM((H, R), F32),
            pltpu.VMEM((NC, R, KC), BF),
            pltpu.VMEM((2, SLOTS, R, KC), BF),
            pltpu.VMEM((2, NC, R // 2, KC), BF),
            pltpu.VMEM((2, NC, R, KC), BF),
            dma((4, NC)), dma((4, NC)), dma((4, NC)), dma((4, NC)),
            dma((2, 3)), dma((4, -(-HK // KC))), dma((NC,)), dma((NC,)),
        ],
        compiler_params=pltpu.CompilerParams(collective_id=0, has_side_effects=True, vmem_limit_bytes=67043328),
        cost_estimate=pl.CostEstimate(flops=8 * T * D * HK, bytes_accessed=8 * D * HK, transcendentals=H * T * T),
    )(x, gain.astype(F32).reshape(U, 1, HEAD), jnp.asarray(freq), wq, wk, wv, wo)


def solution(mesh):
    tokens, columns = P(("dp", "tp"), None), P(None, "tp")
    return jax.shard_map(
        functools.partial(layer, n_tp=mesh.shape["tp"]),
        mesh=mesh,
        in_specs=(tokens, P(None), columns, columns, columns, P("tp", None)),
        out_specs=tokens,
        check_vma=False,
    )
```

```python
import functools

import jax
import jax.numpy as jnp
import numpy as np
from jax import lax
from jax.experimental import pallas as pl
from jax.experimental.pallas import tpu as pltpu
from jax.sharding import PartitionSpec as P

HEAD = 128
THETA = 10000
KC = 512
UC = KC // HEAD
AHEAD = 1
SLOTS = 2
NEG = -1e30
HIDDEN = 2 * NEG
LOG2E = 1.4426950408889634
BF, F32 = jnp.bfloat16, jnp.float32
MESH = pl.DeviceIdType.MESH


def _dot(a, b, ca, cb):
    return lax.dot_general(a, b, (((ca,), (cb,)), ((), ())), preferred_element_type=F32)


def _kernel(x_ref, gain_ref, freq_ref, wq_ref, wk_ref, wv_ref, wo_ref, y_ref, xg, acc, wbuf, cos_s, sin_s, top_s, gain_in, freq_s,
            s_opp, s_full, r_half, ag_send, ag_recv, rs_send, rs_recv, w_sem, wo_sem, x_sem, in_sem, free_sem):
    R, D = x_ref.shape
    n_tp = xg.shape[1] // R
    T = n_tp * R
    U = D // HEAD
    NC = D // KC
    HK = wo_ref.shape[0]
    H = HK // HEAD
    R2 = R // 2
    me = lax.axis_index("tp")
    right, left = lax.rem(me + 1, n_tp), lax.rem(me + n_tp - 1, n_tp)

    OWN, RIGHT, LEFT, OPP = range(4)

    def rows(place, start=0, size=R):
        at = place * R + start
        return pl.ds(at if isinstance(place, int) else pl.multiple_of(at, R2), size)

    def swap(i):
        return jnp.where(i == 2, 3, jnp.where(i == 3, 2, i))

    weights = (wq_ref, wk_ref, wv_ref)

    def w_copy(c, i):
        return pltpu.make_async_copy(
            weights[i].at[pl.ds(pl.multiple_of(c * KC, KC), KC), :],
            wbuf.at[lax.rem(c, 2), :, i * HK : (i + 1) * HK],
            w_sem.at[lax.rem(c, 2), i])

    pieces = [(k, min(KC, HK - k)) for k in range(0, HK, KC)]
    width = len(pieces) * KC
    first_slot = (NC - 2) % 2

    def wo_place(s):
        place = lax.rem(s, 4)
        return place, lax.rem(first_slot + lax.div(place, 2), 2), lax.rem(place, 2) * width

    def wo_copy(s, i):
        place, slot, off = wo_place(s)
        k, size = pieces[i]
        n = lax.rem(s, NC)
        return pltpu.make_async_copy(
            wo_ref.at[k : k + size, pl.ds(pl.multiple_of(n * KC, KC), KC)],
            wbuf.at[slot, 0:size, pl.ds(pl.multiple_of(off + i * KC, KC), KC)],
            wo_sem.at[place, i])

    def wo_start(s):
        for i in range(len(pieces)):
            wo_copy(s, i).start()

    def wo_wait(s):
        for i in range(len(pieces)):
            wo_copy(s, i).wait()

    def wo_cols(s, at, size):
        _, slot, off = wo_place(s)
        return jnp.concatenate(
            [wbuf[slot, 0:ks, pl.ds(pl.multiple_of(off + i * KC + at, HEAD), size)] for i, (k, ks) in enumerate(pieces)], axis=0)

    def seen(here):
        return jnp.concatenate([xg[3 * H + h, here, :] for h in range(H)], axis=1)

    def ag_rows(kind, came):
        if kind == 0:
            return rows(LEFT if came else OWN)
        if kind == 1:
            return rows(RIGHT if came else OWN)
        if kind == 2:
            return rows(OPP if came else LEFT, 0, R2)
        return rows(OPP if came else RIGHT, R2, R2)

    def ag(kind, c):
        src = xg.at[pl.ds(c * UC, UC), ag_rows(kind, False), :]
        dst = xg.at[pl.ds(c * UC, UC), ag_rows(kind, True), :]
        return pltpu.make_async_remote_copy(src, dst, ag_send.at[kind, c], ag_recv.at[kind, c],
                                            device_id={"tp": left if kind % 2 else right}, device_id_type=MESH)

    def rs(kind, n):
        if kind < 2:
            src, dst = s_opp.at[n, kind * R2 : (kind + 1) * R2, :], r_half.at[kind, n]
        else:
            src, dst = s_full.at[kind - 2, lax.rem(n, SLOTS)], xg.at[(kind - 2) * H + n]
        return pltpu.make_async_remote_copy(src, dst, rs_send.at[kind, n], rs_recv.at[kind, n],
                                            device_id={"tp": left if kind % 2 else right}, device_id_type=MESH)

    barrier = pltpu.get_barrier_semaphore()
    for other in (left, right):
        pl.semaphore_signal(barrier, inc=1, device_id={"tp": other}, device_id_type=MESH)

    def x_fetch(side):
        here = rows(OWN, side * R2, R2)

        def start(u, _):
            pltpu.make_async_copy(x_ref.at[side * R2 : (side + 1) * R2, pl.ds(pl.multiple_of(u * HEAD, HEAD), HEAD)], xg.at[u, here, :],
                                  x_sem.at[side]).start()

        lax.fori_loop(0, U, start, None)

    gain_copy = pltpu.make_async_copy(gain_ref, gain_in, in_sem.at[0])
    freq_copy = pltpu.make_async_copy(freq_ref, freq_s, in_sem.at[1])
    x_fetch(0)
    x_fetch(1)
    gain_copy.start()
    freq_copy.start()
    for c in range(2):
        for i in range(3):
            w_copy(c, i).start()
    group = 32

    def sums(g, _):
        here = pl.ds(pl.multiple_of(g * group, group), group)

        def add(u, s):
            t = xg[u, here, :].astype(F32)
            return s + t * t

        s = lax.fori_loop(0, U, add, jnp.zeros((group, HEAD), F32), unroll=4)
        scale = lax.rsqrt(s.sum(-1, keepdims=True) / D + 1e-6)
        acc[0, pl.ds(pl.multiple_of(g * group, group), group), :] = jnp.broadcast_to(scale, (group, HEAD))

    for side in range(2):
        own = xg.at[:, rows(OWN, side * R2, R2), :]
        pltpu.make_async_copy(own, own, x_sem.at[side]).wait()
        lax.fori_loop(side * R2 // group, (side + 1) * R2 // group, sums, None)
    gain_copy.wait()
    for u in range(U):
        acc[1, u * 8 : (u + 1) * 8, :] = jnp.broadcast_to(gain_in[u * HEAD : (u + 1) * HEAD].astype(F32)[None], (8, HEAD))
    pl.semaphore_wait(barrier, 2)

    def norm(c, _):
        def unit(j, _):
            u = c * UC + j
            xg[u, rows(OWN), :] = (xg[u, rows(OWN), :].astype(F32) * acc[0, :R, :] * acc[1, pl.ds(pl.multiple_of(u * 8, 8), 8), :][:1]).astype(BF)

        lax.fori_loop(0, UC, unit, None)

        @pl.when(c <= AHEAD)
        def _():
            ag(0, c).start()
            ag(1, c).start()

    lax.fori_loop(0, NC, norm, None)

    step = 128

    freq_copy.wait()

    def angles(g, _):
        here = pl.ds(pl.multiple_of(g * step, step), step)
        at = g * step
        first = lax.rem(me + swap(lax.div(at, R)), n_tp) * R + lax.rem(at, R)
        place = (lax.broadcasted_iota(jnp.int32, (step, HEAD), 0) + first).astype(F32)
        angle = place * freq_s[...]
        lane = lax.broadcasted_iota(jnp.int32, (step, HEAD), 1)
        sin = jnp.sin(angle)
        cos_s[here, :] = jnp.cos(angle)
        sin_s[here, :] = jnp.where(lane < HEAD // 2, -sin, sin)

    lax.fori_loop(0, T // step, angles, None)

    def clear(u, _):
        acc[u] = jnp.zeros((T, HEAD), F32)

    lax.fori_loop(0, 3 * H, clear, None)

    early, late = slice(0, 3 * R), slice(3 * R, 4 * R)
    wide = 4
    tiles = [(u, min(wide, 3 * H - u)) for u in range(0, 3 * H, wide)]

    def product(c, here, u, count):
        lhs = jnp.concatenate([xg[c * UC + j, here, :] for j in range(UC)], axis=1)
        return jnp.dot(lhs, wbuf[lax.rem(c, 2), :, u * HEAD : (u + count) * HEAD], preferred_element_type=F32)

    def multiply(c, here):
        for u, count in tiles:
            r = product(c, here, u, count)
            for j in range(count):
                acc[u + j, here, :] += r[:, j * HEAD : (j + 1) * HEAD]

    def end(c, here):
        for u, count in tiles:
            r = product(c, here, u, count)
            for j in range(count):
                t = (acc[u + j, here, :] + r[:, j * HEAD : (j + 1) * HEAD]).astype(BF)
                if u + j < 2 * H:
                    t = t.astype(F32)
                    t = (t * cos_s[here, :] + pltpu.roll(t, HEAD // 2, 1) * sin_s[here, :]).astype(BF)
                xg[u + j, here, :] = t

    def near(c):
        ag(0, c).wait_recv()
        ag(1, c).wait_recv()
        ag(2, c).start()
        ag(3, c).start()

    def far(c):
        ag(2, c).wait_recv()
        ag(3, c).wait_recv()

    def w_wait(c):
        for i in range(3):
            w_copy(c, i).wait()

    def gather(c, _):
        near(c)

        @pl.when(c + AHEAD + 1 < NC)
        def _():
            ag(0, c + AHEAD + 1).start()
            ag(1, c + AHEAD + 1).start()

        w_wait(c)
        multiply(c, early)

        @pl.when(c >= 1)
        def _():
            far(c - 1)
            multiply(c - 1, late)
            for i in range(3):
                w_copy(c + 1, i).start()

    lax.fori_loop(0, NC - 1, gather, None)
    near(NC - 1)
    held = -(-3 * H // UC)

    def sent(c, _):
        for kind in range(4):
            ag(kind, c).wait_send()

    lax.fori_loop(0, held, sent, None)
    w_wait(NC - 1)
    end(NC - 1, early)
    far(NC - 2)
    multiply(NC - 2, late)
    far(NC - 1)
    end(NC - 1, late)
    lax.fori_loop(held, NC, sent, None)
    for i in range(4):
        wo_start(i)

    e = HEAD**-0.5 * LOG2E
    ones = jnp.ones((8, R), BF)

    tall = HEAD + 8
    parts = [(q, q // HEAD * 2 * HEAD) for q in range(0, R, HEAD)]

    def mix(h):
        return jnp.concatenate([acc[h, at : at + tall, :] for _, at in parts], axis=1)

    def attend(b, at_q):
        for h in range(H):
            top_s[h : h + 1, :] = jnp.full((1, R), NEG, F32)
            for _, at in parts:
                acc[h, at : at + tall, :] = jnp.zeros((tall, HEAD), F32)

        def block(j, masked):
            keys = rows(swap(lax.rem(j - me + n_tp, n_tp)))
            scores = [_dot(xg[H + h, keys, :], xg[h, at_q, :], 1, 1) for h in range(H)]
            weights, keeps = [], []
            for h, s in enumerate(scores):
                if masked:
                    ok = lax.broadcasted_iota(jnp.int32, (R, R), 1) >= lax.broadcasted_iota(jnp.int32, (R, R), 0)
                    s = jnp.where(ok, s, HIDDEN)
                old = top_s[h : h + 1, :]
                top = jnp.maximum(old, s.max(axis=0, keepdims=True))
                top_s[h : h + 1, :] = top
                weights.append(jnp.exp2((s - top) * e).astype(BF))
                keeps.append(jnp.exp2((old - top) * e))
            for h, (p, keep) in enumerate(zip(weights, keeps)):
                values = jnp.concatenate([xg[2 * H + h, keys, :].T, ones], axis=0)
                new = mix(h) * keep + _dot(values, p, 1, 0)
                for q, at in parts:
                    acc[h, at : at + tall, :] = new[:, q : q + HEAD]

        lax.fori_loop(0, b, lambda j, _: block(j, False), None)
        block(b, True)
        for h in range(H):
            got = mix(h)
            xg[3 * H + h, at_q, :] = (got[:HEAD] * (1 / got[HEAD : HEAD + 1])).T.astype(BF)

    half = KC // 2

    def send_opp(n, _):
        wo_wait(n)
        for at in (0, half):
            s_opp[n, :, at : at + half] = jnp.dot(seen(late), wo_cols(n, at, half), preferred_element_type=F32).astype(BF)
        rs(0, n).start()
        rs(1, n).start()
        wo_start(n + 4)

    def attention(i, _):
        place = jnp.where(i == 0, OPP, jnp.where(i == 3, OWN, i))
        attend(lax.rem(me + swap(place), n_tp), rows(place))

        @pl.when(i == 0)
        def _():
            lax.fori_loop(0, NC, send_opp, None)

    lax.fori_loop(0, n_tp, attention, None)

    for k, other in enumerate((left, right)):
        pl.semaphore_signal(free_sem.at[k], inc=1, device_id={"tp": other}, device_id_type=MESH)

    def x_tile(n, j):
        return pltpu.make_async_copy(x_ref.at[:, pl.ds(pl.multiple_of(n * KC + j * HEAD, HEAD), HEAD)], xg.at[2 * H + n, rows(j), :], x_sem.at[n])

    def x_start(n, _):
        for j in range(UC):
            x_tile(n, j).start()

    lax.fori_loop(0, NC, x_start, None)
    for k in range(2):
        pl.semaphore_wait(free_sem.at[k], 1)

    def send_full(n):
        wo_wait(n + NC)
        rs(0, n).wait_recv()
        rs(1, n).wait_recv()

        @pl.when(n >= SLOTS)
        def _():
            rs(2, n - SLOTS).wait_send()
            rs(3, n - SLOTS).wait_send()

        slot = lax.rem(n, SLOTS)
        lhs = seen(early)
        for at in (0, half):
            r = jnp.dot(lhs, wo_cols(n + NC, at, half), preferred_element_type=F32)
            for j in range(half // HEAD):
                own, to_right, to_left = (r[b * R : (b + 1) * R, j * HEAD : (j + 1) * HEAD] for b in range(3))
                cols, first = slice(at + j * HEAD, at + (j + 1) * HEAD), (at // HEAD + j) * R
                upper, lower = slice(first, first + R2), slice(first + R2, first + R)
                s_full[0, slot, upper, :] = (to_right[:R2] + r_half[0, n, :, cols].astype(F32)).astype(BF)
                s_full[0, slot, lower, :] = to_right[R2:].astype(BF)
                s_full[1, slot, upper, :] = to_left[:R2].astype(BF)
                s_full[1, slot, lower, :] = (to_left[R2:] + r_half[1, n, :, cols].astype(F32)).astype(BF)
                acc[n, rows(at // HEAD + j), :] = own
        rs(2, n).start()
        rs(3, n).start()

        @pl.when(n + 4 < NC)
        def _():
            wo_start(n + NC + 4)

    def finish(n):
        rs(2, n).wait_recv()
        rs(3, n).wait_recv()
        tile = xg.at[2 * H + n]
        pltpu.make_async_copy(tile, tile, x_sem.at[n]).wait()
        for j in range(UC):
            here = rows(j)
            total = acc[n, here, :] + xg[n, here, :].astype(F32) + xg[H + n, here, :].astype(F32)
            y_ref[:, pl.ds(pl.multiple_of(n * KC + j * HEAD, HEAD), HEAD)] = (xg[2 * H + n, here, :].astype(F32) + total).astype(BF)

    def both(n, _):
        @pl.when(n < NC)
        def _():
            send_full(n)

        @pl.when(n >= SLOTS)
        def _():
            finish(n - SLOTS)

    lax.fori_loop(0, NC + SLOTS, both, None)

    def close(n, _):
        rs(0, n).wait_send()
        rs(1, n).wait_send()

        @pl.when(n >= NC - SLOTS)
        def _():
            rs(2, n).wait_send()
            rs(3, n).wait_send()

    lax.fori_loop(0, NC, close, None)


PARTS = 4


def _move(a_ref, b_ref, sem):
    size = a_ref.shape[0] // PARTS
    copies = [pltpu.make_async_copy(a_ref.at[i * size : (i + 1) * size], b_ref.at[i * size : (i + 1) * size], sem.at[i]) for i in range(PARTS)]
    for c in copies:
        c.start()
    for c in copies:
        c.wait()


def moved(a):
    return pl.pallas_call(
        _move,
        out_shape=jax.ShapeDtypeStruct(a.shape, a.dtype),
        in_specs=[pl.BlockSpec(memory_space=pltpu.VMEM)],
        out_specs=pl.BlockSpec(memory_space=pl.ANY),
        scratch_shapes=[pltpu.SemaphoreType.DMA((PARTS,))],
        compiler_params=pltpu.CompilerParams(vmem_limit_bytes=8 * 2**20),
        cost_estimate=pl.CostEstimate(flops=1, bytes_accessed=4 * a.size, transcendentals=0),
    )(a)


def layer(x, gain, wq, wk, wv, wo, n_tp):
    R, D = x.shape
    HK = wo.shape[0]
    H = HK // HEAD
    T, U, NC = n_tp * R, D // HEAD, D // KC
    half = HEAD // 2
    freq = np.tile(np.float32(THETA) ** (-np.arange(half, dtype=np.float32) / np.float32(half)), 2)[None]
    any_ = pl.BlockSpec(memory_space=pl.ANY)
    dma = pltpu.SemaphoreType.DMA
    y = pl.pallas_call(
        _kernel,
        out_shape=pltpu.VMEM((R, D), BF),
        in_specs=[any_] * 7,
        out_specs=pl.BlockSpec(memory_space=pltpu.VMEM),
        scratch_shapes=[
            pltpu.VMEM((U, T, HEAD), BF),
            pltpu.VMEM((3 * H, T, HEAD), F32),
            pltpu.VMEM((2, KC, 3 * HK), BF),
            pltpu.VMEM((T, HEAD), F32),
            pltpu.VMEM((T, HEAD), F32),
            pltpu.VMEM((H, R), F32),
            pltpu.VMEM((D,), BF),
            pltpu.VMEM((1, HEAD), F32),
            pltpu.VMEM((NC, R, KC), BF),
            pltpu.VMEM((2, SLOTS, UC * R, HEAD), BF),
            pltpu.VMEM((2, NC, R // 2, KC), BF),
            dma((4, NC)), dma((4, NC)), dma((4, NC)), dma((4, NC)),
            dma((2, 3)), dma((4, -(-HK // KC))), dma((NC,)), dma((2,)), pltpu.SemaphoreType.REGULAR((2,)),
        ],
        compiler_params=pltpu.CompilerParams(collective_id=0, has_side_effects=True, vmem_limit_bytes=63000000),
        cost_estimate=pl.CostEstimate(flops=8 * T * D * HK, bytes_accessed=8 * D * HK, transcendentals=H * T * T),
    )(x, gain, jnp.asarray(freq), wq, wk, wv, wo)
    return moved(y)


def solution(mesh):
    tokens, columns = P(("dp", "tp"), None), P(None, "tp")
    return jax.shard_map(
        functools.partial(layer, n_tp=mesh.shape["tp"]),
        mesh=mesh,
        in_specs=(tokens, P(None), columns, columns, columns, P("tp", None)),
        out_specs=tokens,
        check_vma=False,
    )
```

```python
import functools

import jax
import jax.numpy as jnp
import numpy as np
from jax import lax
from jax.experimental import pallas as pl
from jax.experimental.pallas import tpu as pltpu
from jax.sharding import PartitionSpec as P

HEAD = 128
THETA = 10000
KC = 512
UC = KC // HEAD
AHEAD = 1
SLOTS = 2
NEG = -1e30
HIDDEN = 2 * NEG
LOG2E = 1.4426950408889634
BF, F32 = jnp.bfloat16, jnp.float32
MESH = pl.DeviceIdType.MESH


def _dot(a, b, ca, cb):
    return lax.dot_general(a, b, (((ca,), (cb,)), ((), ())), preferred_element_type=F32)


def _kernel(x_ref, gain_ref, freq_ref, wq_ref, wk_ref, wv_ref, wo_ref, y_ref, xg, acc, wbuf, cos_s, sin_s, top_s, gain_in, freq_s,
            s_opp, s_full, r_half, ag_send, ag_recv, rs_send, rs_recv, w_sem, wo_sem, x_sem, in_sem, free_sem):
    R, D = x_ref.shape
    n_tp = xg.shape[1] // R
    T = n_tp * R
    U = D // HEAD
    NC = D // KC
    HK = wo_ref.shape[0]
    H = HK // HEAD
    R2 = R // 2
    me = lax.axis_index("tp")
    right, left = lax.rem(me + 1, n_tp), lax.rem(me + n_tp - 1, n_tp)

    OWN, RIGHT, LEFT, OPP = range(4)

    def rows(place, start=0, size=R):
        at = place * R + start
        return pl.ds(at if isinstance(place, int) else pl.multiple_of(at, R2), size)

    def swap(i):
        return jnp.where(i == 2, 3, jnp.where(i == 3, 2, i))

    weights = (wq_ref, wk_ref, wv_ref)

    def w_copy(c, i):
        return pltpu.make_async_copy(
            weights[i].at[pl.ds(pl.multiple_of(c * KC, KC), KC), :],
            wbuf.at[lax.rem(c, 2), :, i * HK : (i + 1) * HK],
            w_sem.at[lax.rem(c, 2), i])

    pieces = [(k, min(KC, HK - k)) for k in range(0, HK, KC)]
    width = len(pieces) * KC
    first_slot = (NC - 2) % 2

    def wo_place(s):
        place = lax.rem(s, 4)
        return place, lax.rem(first_slot + lax.div(place, 2), 2), lax.rem(place, 2) * width

    def wo_copy(s, i):
        place, slot, off = wo_place(s)
        k, size = pieces[i]
        n = lax.rem(s, NC)
        return pltpu.make_async_copy(
            wo_ref.at[k : k + size, pl.ds(pl.multiple_of(n * KC, KC), KC)],
            wbuf.at[slot, 0:size, pl.ds(pl.multiple_of(off + i * KC, KC), KC)],
            wo_sem.at[place, i])

    def wo_start(s):
        for i in range(len(pieces)):
            wo_copy(s, i).start()

    def wo_wait(s):
        for i in range(len(pieces)):
            wo_copy(s, i).wait()

    def wo_cols(s, at, size):
        _, slot, off = wo_place(s)
        return jnp.concatenate(
            [wbuf[slot, 0:ks, pl.ds(pl.multiple_of(off + i * KC + at, HEAD), size)] for i, (k, ks) in enumerate(pieces)], axis=0)

    def seen(here):
        return jnp.concatenate([xg[3 * H + h, here, :] for h in range(H)], axis=1)

    def ag_rows(kind, came):
        if kind == 0:
            return rows(LEFT if came else OWN)
        if kind == 1:
            return rows(RIGHT if came else OWN)
        if kind == 2:
            return rows(OPP if came else LEFT, 0, R2)
        return rows(OPP if came else RIGHT, R2, R2)

    def ag(kind, c):
        src = xg.at[pl.ds(c * UC, UC), ag_rows(kind, False), :]
        dst = xg.at[pl.ds(c * UC, UC), ag_rows(kind, True), :]
        return pltpu.make_async_remote_copy(src, dst, ag_send.at[kind, c], ag_recv.at[kind, c],
                                            device_id={"tp": left if kind % 2 else right}, device_id_type=MESH)

    R4 = R // 4

    def rs(kind, n):
        way = lax.rem(kind, 2)
        if isinstance(kind, int) and kind >= 4:
            src, dst = s_full.at[kind - 4, lax.rem(n, SLOTS)], xg.at[(kind - 4) * H + n]
        else:
            side = lax.div(kind, 2)
            src = s_opp.at[n, pl.ds(pl.multiple_of(side * R2 + way * R4, R4), R4), :]
            dst = r_half.at[way, n, pl.ds(pl.multiple_of(side * R4, R4), R4), :]
        return pltpu.make_async_remote_copy(src, dst, rs_send.at[kind, n], rs_recv.at[kind, n],
                                            device_id={"tp": jnp.where(way == 0, right, left)}, device_id_type=MESH)

    barrier = pltpu.get_barrier_semaphore()
    for other in (left, right):
        pl.semaphore_signal(barrier, inc=1, device_id={"tp": other}, device_id_type=MESH)

    group = 32

    def cols(u):
        return pl.ds(pl.multiple_of(u * HEAD, HEAD), HEAD)

    def x_copy(g):
        here = pl.ds(pl.multiple_of(g * group, group), group)
        return pltpu.make_async_copy(x_ref.at[here, :], y_ref.at[here, :], x_sem.at[g])

    gain_copy = pltpu.make_async_copy(gain_ref, gain_in, in_sem.at[0])
    freq_copy = pltpu.make_async_copy(freq_ref, freq_s, in_sem.at[1])
    for g in range(R // group):
        x_copy(g).start()
    gain_copy.start()
    freq_copy.start()
    for c in range(2):
        for i in range(3):
            w_copy(c, i).start()
    def sums(g, _):
        x_copy(g).wait()
        here = pl.ds(pl.multiple_of(g * group, group), group)

        def add(u, s):
            t = y_ref[here, cols(u)].astype(F32)
            return s + t * t

        s = lax.fori_loop(0, U, add, jnp.zeros((group, HEAD), F32), unroll=4)
        scale = lax.rsqrt(s.sum(-1, keepdims=True) / D + 1e-6)
        acc[0, pl.ds(pl.multiple_of(g * group, group), group), :] = jnp.broadcast_to(scale, (group, HEAD))

    lax.fori_loop(0, R // group, sums, None)
    gain_copy.wait()
    for u in range(U):
        acc[1, u * 8 : (u + 1) * 8, :] = jnp.broadcast_to(gain_in[u * HEAD : (u + 1) * HEAD].astype(F32)[None], (8, HEAD))
    pl.semaphore_wait(barrier, 2)

    def norm(c, _):
        def unit(j, _):
            u = c * UC + j
            xg[u, rows(OWN), :] = (y_ref[:, cols(u)].astype(F32) * acc[0, :R, :] * acc[1, pl.ds(pl.multiple_of(u * 8, 8), 8), :][:1]).astype(BF)

        lax.fori_loop(0, UC, unit, None)

        @pl.when(c <= AHEAD)
        def _():
            ag(0, c).start()
            ag(1, c).start()

    lax.fori_loop(0, NC, norm, None)

    step = 128

    freq_copy.wait()

    def angles(g, _):
        here = pl.ds(pl.multiple_of(g * step, step), step)
        at = g * step
        first = lax.rem(me + swap(lax.div(at, R)), n_tp) * R + lax.rem(at, R)
        place = (lax.broadcasted_iota(jnp.int32, (step, HEAD), 0) + first).astype(F32)
        angle = place * freq_s[...]
        lane = lax.broadcasted_iota(jnp.int32, (step, HEAD), 1)
        sin = jnp.sin(angle)
        cos_s[here, :] = jnp.cos(angle)
        sin_s[here, :] = jnp.where(lane < HEAD // 2, -sin, sin)

    lax.fori_loop(0, T // step, angles, None)

    def clear(u, _):
        acc[u] = jnp.zeros((T, HEAD), F32)

    lax.fori_loop(0, 3 * H, clear, None)

    early, late = slice(0, 3 * R), slice(3 * R, 4 * R)
    wide = 4
    tiles = [(u, min(wide, 3 * H - u)) for u in range(0, 3 * H, wide)]

    def product(c, here, u, count):
        lhs = jnp.concatenate([xg[c * UC + j, here, :] for j in range(UC)], axis=1)
        return jnp.dot(lhs, wbuf[lax.rem(c, 2), :, u * HEAD : (u + count) * HEAD], preferred_element_type=F32)

    def multiply(c, here):
        for u, count in tiles:
            r = product(c, here, u, count)
            for j in range(count):
                acc[u + j, here, :] += r[:, j * HEAD : (j + 1) * HEAD]

    def end(c, here):
        for u, count in tiles:
            r = product(c, here, u, count)
            for j in range(count):
                t = (acc[u + j, here, :] + r[:, j * HEAD : (j + 1) * HEAD]).astype(BF)
                if u + j < 2 * H:
                    t = t.astype(F32)
                    t = (t * cos_s[here, :] + pltpu.roll(t, HEAD // 2, 1) * sin_s[here, :]).astype(BF)
                xg[u + j, here, :] = t

    def near(c):
        ag(0, c).wait_recv()
        ag(1, c).wait_recv()
        ag(2, c).start()
        ag(3, c).start()

    def far(c):
        ag(2, c).wait_recv()
        ag(3, c).wait_recv()

    def w_wait(c):
        for i in range(3):
            w_copy(c, i).wait()

    def gather(c, _):
        near(c)

        @pl.when(c + AHEAD + 1 < NC)
        def _():
            ag(0, c + AHEAD + 1).start()
            ag(1, c + AHEAD + 1).start()

        w_wait(c)
        multiply(c, early)

        @pl.when(c >= 1)
        def _():
            far(c - 1)
            multiply(c - 1, late)
            for i in range(3):
                w_copy(c + 1, i).start()

    lax.fori_loop(0, NC - 1, gather, None)
    near(NC - 1)
    held = -(-3 * H // UC)

    def sent(c, _):
        for kind in range(4):
            ag(kind, c).wait_send()

    lax.fori_loop(0, held, sent, None)
    w_wait(NC - 1)
    end(NC - 1, early)
    far(NC - 2)
    multiply(NC - 2, late)
    far(NC - 1)
    end(NC - 1, late)
    lax.fori_loop(held, NC, sent, None)
    for i in range(4):
        wo_start(i)

    e = HEAD**-0.5 * LOG2E
    ones = jnp.ones((8, R), BF)

    tall = HEAD + 8

    def attend(b, at_q, first, size):
        parts = [(q, q // HEAD * 2 * HEAD, min(HEAD, size - q)) for q in range(0, size, HEAD)]

        def mix(h):
            return jnp.concatenate([acc[h, at : at + tall, :w] for _, at, w in parts], axis=1)

        for h in range(H):
            top_s[h : h + 1, :size] = jnp.full((1, size), NEG, F32)
            for _, at, w in parts:
                acc[h, at : at + tall, :w] = jnp.zeros((tall, w), F32)

        def block(j, masked):
            keys = rows(swap(lax.rem(j - me + n_tp, n_tp)))
            scores = [_dot(xg[H + h, keys, :], xg[h, at_q, :], 1, 1) for h in range(H)]
            weights, keeps = [], []
            for h, s in enumerate(scores):
                if masked:
                    ok = lax.broadcasted_iota(jnp.int32, (R, size), 1) + first >= lax.broadcasted_iota(jnp.int32, (R, size), 0)
                    s = jnp.where(ok, s, HIDDEN)
                old = top_s[h : h + 1, :size]
                top = jnp.maximum(old, s.max(axis=0, keepdims=True))
                top_s[h : h + 1, :size] = top
                weights.append(jnp.exp2((s - top) * e).astype(BF))
                keeps.append(jnp.exp2((old - top) * e))
            for h, (p, keep) in enumerate(zip(weights, keeps)):
                values = jnp.concatenate([xg[2 * H + h, keys, :].T, ones], axis=0)
                new = mix(h) * keep + _dot(values, p, 1, 0)
                for q, at, w in parts:
                    acc[h, at : at + tall, :w] = new[:, q : q + w]

        lax.fori_loop(0, b, lambda j, _: block(j, False), None)
        block(b, True)
        for h in range(H):
            got = mix(h)
            xg[3 * H + h, at_q, :] = (got[:HEAD] * (1 / got[HEAD : HEAD + 1])).T.astype(BF)

    half = KC // 2

    def opp_tile(n, first, size):
        for at in (0, half):
            r = jnp.dot(seen(rows(OPP, first, size)), wo_cols(n, at, half), preferred_element_type=F32)
            s_opp[n, pl.ds(first, size), at : at + half] = r.astype(BF)

    FIRST = min(4, NC)

    def opp_half(side, _):
        first = pl.multiple_of(side * R2, R2)
        attend(lax.rem(me + 2, n_tp), rows(OPP, first, R2), first, R2)

        def tile(n, _):
            @pl.when(side == 0)
            def _():
                wo_wait(n)

            opp_tile(n, first, R2)
            for way in range(2):
                rs(2 * side + way, n).start()

            @pl.when(side == 1)
            def _():
                wo_start(n + 4)

        lax.fori_loop(0, FIRST, tile, None)

    def opp_whole(n, _):
        wo_wait(n)
        opp_tile(n, 0, R)
        for kind in range(4):
            rs(kind, n).start()
        wo_start(n + 4)

    lax.fori_loop(0, 2, opp_half, None)
    lax.fori_loop(FIRST, NC, opp_whole, None)

    def others(i, _):
        place = lax.rem(i + 1, 3)
        attend(lax.rem(me + swap(place), n_tp), rows(place), 0, R)

    lax.fori_loop(0, 3, others, None)

    for k, other in enumerate((left, right)):
        pl.semaphore_signal(free_sem.at[k], inc=1, device_id={"tp": other}, device_id_type=MESH)

    for k in range(2):
        pl.semaphore_wait(free_sem.at[k], 1)

    def send_full(n):
        wo_wait(n + NC)
        for kind in range(4):
            rs(kind, n).wait_recv()

        @pl.when(n >= SLOTS)
        def _():
            rs(4, n - SLOTS).wait_send()
            rs(5, n - SLOTS).wait_send()

        slot = lax.rem(n, SLOTS)
        lhs = seen(early)
        for at in (0, half):
            r = jnp.dot(lhs, wo_cols(n + NC, at, half), preferred_element_type=F32)
            for j in range(half // HEAD):
                own, to_right, to_left = (r[b * R : (b + 1) * R, j * HEAD : (j + 1) * HEAD] for b in range(3))
                here, first = slice(at + j * HEAD, at + (j + 1) * HEAD), (at // HEAD + j) * R
                for q in range(4):
                    quarter, came = slice(q * R4, (q + 1) * R4), r_half[q % 2, n, q // 2 * R4 : (q // 2 + 1) * R4, here].astype(F32)
                    for way, t in enumerate((to_right[quarter], to_left[quarter])):
                        s_full[way, slot, first + q * R4 : first + (q + 1) * R4, :] = (t + came if q % 2 == way else t).astype(BF)
                acc[n, rows(at // HEAD + j), :] = own
        rs(4, n).start()
        rs(5, n).start()

        @pl.when(n + 4 < NC)
        def _():
            wo_start(n + NC + 4)

    def finish(n):
        rs(4, n).wait_recv()
        rs(5, n).wait_recv()
        for j in range(UC):
            here = rows(j)
            total = acc[n, here, :] + xg[n, here, :].astype(F32) + xg[H + n, here, :].astype(F32)
            y_ref[:, cols(n * UC + j)] = (y_ref[:, cols(n * UC + j)].astype(F32) + total).astype(BF)

    def both(n, _):
        @pl.when(n < NC)
        def _():
            send_full(n)

        @pl.when(n >= SLOTS)
        def _():
            finish(n - SLOTS)

    lax.fori_loop(0, NC + SLOTS, both, None)

    def close(n, _):
        for kind in range(4):
            rs(kind, n).wait_send()

        @pl.when(n >= NC - SLOTS)
        def _():
            rs(4, n).wait_send()
            rs(5, n).wait_send()

    lax.fori_loop(0, NC, close, None)


PARTS = 4


def _move(a_ref, b_ref, sem):
    size = a_ref.shape[0] // PARTS
    copies = [pltpu.make_async_copy(a_ref.at[i * size : (i + 1) * size], b_ref.at[i * size : (i + 1) * size], sem.at[i]) for i in range(PARTS)]
    for c in copies:
        c.start()
    for c in copies:
        c.wait()


def moved(a):
    return pl.pallas_call(
        _move,
        out_shape=jax.ShapeDtypeStruct(a.shape, a.dtype),
        in_specs=[pl.BlockSpec(memory_space=pltpu.VMEM)],
        out_specs=pl.BlockSpec(memory_space=pl.ANY),
        scratch_shapes=[pltpu.SemaphoreType.DMA((PARTS,))],
        compiler_params=pltpu.CompilerParams(vmem_limit_bytes=8 * 2**20),
        cost_estimate=pl.CostEstimate(flops=1, bytes_accessed=4 * a.size, transcendentals=0),
    )(a)


def layer(x, gain, wq, wk, wv, wo, n_tp):
    R, D = x.shape
    HK = wo.shape[0]
    H = HK // HEAD
    T, U, NC = n_tp * R, D // HEAD, D // KC
    half = HEAD // 2
    freq = np.tile(np.float32(THETA) ** (-np.arange(half, dtype=np.float32) / np.float32(half)), 2)[None]
    any_ = pl.BlockSpec(memory_space=pl.ANY)
    dma = pltpu.SemaphoreType.DMA
    y = pl.pallas_call(
        _kernel,
        out_shape=pltpu.VMEM((R, D), BF),
        in_specs=[any_] * 7,
        out_specs=pl.BlockSpec(memory_space=pltpu.VMEM),
        scratch_shapes=[
            pltpu.VMEM((U, T, HEAD), BF),
            pltpu.VMEM((3 * H, T, HEAD), F32),
            pltpu.VMEM((2, KC, 3 * HK), BF),
            pltpu.VMEM((T, HEAD), F32),
            pltpu.VMEM((T, HEAD), F32),
            pltpu.VMEM((H, R), F32),
            pltpu.VMEM((D,), BF),
            pltpu.VMEM((1, HEAD), F32),
            pltpu.VMEM((NC, R, KC), BF),
            pltpu.VMEM((2, SLOTS, UC * R, HEAD), BF),
            pltpu.VMEM((2, NC, R // 2, KC), BF),
            dma((4, NC)), dma((4, NC)), dma((6, NC)), dma((6, NC)),
            dma((2, 3)), dma((4, -(-HK // KC))), dma((R // 32,)), dma((2,)), pltpu.SemaphoreType.REGULAR((2,)),
        ],
        compiler_params=pltpu.CompilerParams(collective_id=0, has_side_effects=True, vmem_limit_bytes=63000000),
        cost_estimate=pl.CostEstimate(flops=8 * T * D * HK, bytes_accessed=8 * D * HK, transcendentals=H * T * T),
    )(x, gain, jnp.asarray(freq), wq, wk, wv, wo)
    return moved(y)


def solution(mesh):
    tokens, columns = P(("dp", "tp"), None), P(None, "tp")
    return jax.shard_map(
        functools.partial(layer, n_tp=mesh.shape["tp"]),
        mesh=mesh,
        in_specs=(tokens, P(None), columns, columns, columns, P("tp", None)),
        out_specs=tokens,
        check_vma=False,
    )
```

```python
import functools

import jax
import jax.numpy as jnp
import numpy as np
from jax import lax
from jax.experimental import pallas as pl
from jax.experimental.pallas import tpu as pltpu
from jax.sharding import PartitionSpec as P

HEAD = 128
THETA = 10000
KC = 512
UC = KC // HEAD
AHEAD = 1
SLOTS = 2
NEG = -1e30
HIDDEN = 2 * NEG
LOG2E = 1.4426950408889634
BF, F32 = jnp.bfloat16, jnp.float32
MESH = pl.DeviceIdType.MESH


def _dot(a, b, ca, cb):
    return lax.dot_general(a, b, (((ca,), (cb,)), ((), ())), preferred_element_type=F32)


def _kernel(x_ref, gain_ref, freq_ref, wq_ref, wk_ref, wv_ref, wo_ref, y_ref, xg, acc, wbuf, cos_s, sin_s, top_s, gain_in, freq_s,
            s_opp, s_full, r_half, ag_send, ag_recv, rs_send, rs_recv, w_sem, wo_sem, x_sem, in_sem, free_sem):
    R, D = x_ref.shape
    n_tp = xg.shape[1] // R
    T = n_tp * R
    U = D // HEAD
    NC = D // KC
    HK = wo_ref.shape[0]
    H = HK // HEAD
    R2 = R // 2
    me = lax.axis_index("tp")
    right, left = lax.rem(me + 1, n_tp), lax.rem(me + n_tp - 1, n_tp)

    OWN, RIGHT, LEFT, OPP = range(4)

    def rows(place, start=0, size=R):
        at = place * R + start
        return pl.ds(at if isinstance(place, int) else pl.multiple_of(at, R2), size)

    def swap(i):
        return jnp.where(i == 2, 3, jnp.where(i == 3, 2, i))

    weights = (wq_ref, wk_ref, wv_ref)

    def w_copy(c, i):
        return pltpu.make_async_copy(
            weights[i].at[pl.ds(pl.multiple_of(c * KC, KC), KC), :],
            wbuf.at[lax.rem(c, 2), :, i * HK : (i + 1) * HK],
            w_sem.at[lax.rem(c, 2), i])

    pieces = [(k, min(KC, HK - k)) for k in range(0, HK, KC)]
    width = len(pieces) * KC
    first_slot = (NC - 2) % 2

    def wo_place(s):
        place = lax.rem(s, 4)
        return place, lax.rem(first_slot + lax.div(place, 2), 2), lax.rem(place, 2) * width

    FIRST = min(6, NC)

    def wo_copy(s, i):
        place, slot, off = wo_place(s)
        k, size = pieces[i]
        n = jnp.where(s < FIRST, s, jnp.where(s < FIRST + NC, s - FIRST, s - FIRST - NC))
        return pltpu.make_async_copy(
            wo_ref.at[k : k + size, pl.ds(pl.multiple_of(n * KC, KC), KC)],
            wbuf.at[slot, 0:size, pl.ds(pl.multiple_of(off + i * KC, KC), KC)],
            wo_sem.at[place, i])

    def wo_start(s):
        for i in range(len(pieces)):
            wo_copy(s, i).start()

    def wo_wait(s):
        for i in range(len(pieces)):
            wo_copy(s, i).wait()

    def wo_cols(s, at, size):
        _, slot, off = wo_place(s)
        return jnp.concatenate(
            [wbuf[slot, 0:ks, pl.ds(pl.multiple_of(off + i * KC + at, HEAD), size)] for i, (k, ks) in enumerate(pieces)], axis=0)

    def seen(here):
        return jnp.concatenate([xg[3 * H + h, here, :] for h in range(H)], axis=1)

    def ag_rows(kind, came):
        if kind == 0:
            return rows(LEFT if came else OWN)
        if kind == 1:
            return rows(RIGHT if came else OWN)
        if kind == 2:
            return rows(OPP if came else LEFT, 0, R2)
        return rows(OPP if came else RIGHT, R2, R2)

    def ag(kind, c):
        src = xg.at[pl.ds(c * UC, UC), ag_rows(kind, False), :]
        dst = xg.at[pl.ds(c * UC, UC), ag_rows(kind, True), :]
        return pltpu.make_async_remote_copy(src, dst, ag_send.at[kind, c], ag_recv.at[kind, c],
                                            device_id={"tp": left if kind % 2 else right}, device_id_type=MESH)

    R4 = R // 4

    def rs(kind, n):
        way = lax.rem(kind, 2)
        if isinstance(kind, int) and kind >= 4:
            src, dst = s_full.at[kind - 4, lax.rem(n, SLOTS)], xg.at[(kind - 4) * H + n]
        else:
            side = lax.div(kind, 2)
            src = s_opp.at[n, pl.ds(pl.multiple_of(side * R2 + way * R4, R4), R4), :]
            dst = r_half.at[way, n, pl.ds(pl.multiple_of(side * R4, R4), R4), :]
        return pltpu.make_async_remote_copy(src, dst, rs_send.at[kind, n], rs_recv.at[kind, n],
                                            device_id={"tp": jnp.where(way == 0, right, left)}, device_id_type=MESH)

    barrier = pltpu.get_barrier_semaphore()
    for other in (left, right):
        pl.semaphore_signal(barrier, inc=1, device_id={"tp": other}, device_id_type=MESH)

    group = 32

    def cols(u):
        return pl.ds(pl.multiple_of(u * HEAD, HEAD), HEAD)

    def x_copy(g):
        here = pl.ds(pl.multiple_of(g * group, group), group)
        return pltpu.make_async_copy(x_ref.at[here, :], y_ref.at[here, :], x_sem.at[g])

    gain_copy = pltpu.make_async_copy(gain_ref, gain_in, in_sem.at[0])
    freq_copy = pltpu.make_async_copy(freq_ref, freq_s, in_sem.at[1])
    for g in range(R // group):
        x_copy(g).start()
    gain_copy.start()
    freq_copy.start()
    for c in range(2):
        for i in range(3):
            w_copy(c, i).start()
    def sums(g, _):
        x_copy(g).wait()
        here = pl.ds(pl.multiple_of(g * group, group), group)

        def add(u, s):
            t = y_ref[here, cols(u)].astype(F32)
            return s + t * t

        s = lax.fori_loop(0, U, add, jnp.zeros((group, HEAD), F32), unroll=26)
        scale = lax.rsqrt(s.sum(-1, keepdims=True) / D + 1e-6)
        acc[0, pl.ds(pl.multiple_of(g * group, group), group), :] = jnp.broadcast_to(scale, (group, HEAD))

    lax.fori_loop(0, R // group, sums, None)
    gain_copy.wait()
    for u in range(U):
        acc[1, u * 8 : (u + 1) * 8, :] = jnp.broadcast_to(gain_in[u * HEAD : (u + 1) * HEAD].astype(F32)[None], (8, HEAD))
    pl.semaphore_wait(barrier, 2)

    def norm(c, _):
        def unit(j, _):
            u = c * UC + j
            xg[u, rows(OWN), :] = (y_ref[:, cols(u)].astype(F32) * acc[0, :R, :] * acc[1, pl.ds(pl.multiple_of(u * 8, 8), 8), :][:1]).astype(BF)

        lax.fori_loop(0, UC, unit, None)

        @pl.when(c <= AHEAD)
        def _():
            ag(0, c).start()
            ag(1, c).start()

    lax.fori_loop(0, NC, norm, None)

    step = 128

    freq_copy.wait()

    def angles(g, _):
        here = pl.ds(pl.multiple_of(g * step, step), step)
        at = g * step
        first = lax.rem(me + swap(lax.div(at, R)), n_tp) * R + lax.rem(at, R)
        place = (lax.broadcasted_iota(jnp.int32, (step, HEAD), 0) + first).astype(F32)
        angle = place * freq_s[...]
        lane = lax.broadcasted_iota(jnp.int32, (step, HEAD), 1)
        sin = jnp.sin(angle)
        cos_s[here, :] = jnp.cos(angle)
        sin_s[here, :] = jnp.where(lane < HEAD // 2, -sin, sin)

    lax.fori_loop(0, T // step, angles, None)

    def clear(u, _):
        acc[u] = jnp.zeros((T, HEAD), F32)

    lax.fori_loop(0, 3 * H, clear, None)

    early, late = slice(0, 3 * R), slice(3 * R, 4 * R)
    wide = 4
    tiles = [(u, min(wide, 3 * H - u)) for u in range(0, 3 * H, wide)]

    def product(chunks, here, u, count):
        lhs = jnp.concatenate([xg[c * UC + j, here, :] for c in chunks for j in range(UC)], axis=1)
        rhs = jnp.concatenate([wbuf[lax.rem(c, 2), :, u * HEAD : (u + count) * HEAD] for c in chunks], axis=0)
        return jnp.dot(lhs, rhs, preferred_element_type=F32)

    def multiply(chunks, here):
        for u, count in tiles:
            r = product(chunks, here, u, count)
            for j in range(count):
                acc[u + j, here, :] += r[:, j * HEAD : (j + 1) * HEAD]

    def end(chunks, here):
        for u, count in tiles:
            r = product(chunks, here, u, count)
            for j in range(count):
                t = (acc[u + j, here, :] + r[:, j * HEAD : (j + 1) * HEAD]).astype(BF)
                if u + j < 2 * H:
                    t = t.astype(F32)
                    t = (t * cos_s[here, :] + pltpu.roll(t, HEAD // 2, 1) * sin_s[here, :]).astype(BF)
                xg[u + j, here, :] = t

    def near(c):
        ag(0, c).wait_recv()
        ag(1, c).wait_recv()
        ag(2, c).start()
        ag(3, c).start()

    def far(c):
        ag(2, c).wait_recv()
        ag(3, c).wait_recv()

    def w_wait(c):
        for i in range(3):
            w_copy(c, i).wait()

    def gather(c, _):
        near(c)

        @pl.when(c + AHEAD + 1 < NC)
        def _():
            ag(0, c + AHEAD + 1).start()
            ag(1, c + AHEAD + 1).start()

        w_wait(c)
        multiply([c], early)

        @pl.when(c >= 1)
        def _():
            far(c - 1)
            multiply([c - 1], late)
            for i in range(3):
                w_copy(c + 1, i).start()

    lax.fori_loop(0, NC - 1, gather, None)
    near(NC - 1)
    held = -(-3 * H // UC)

    def sent(c, _):
        for kind in range(4):
            ag(kind, c).wait_send()

    lax.fori_loop(0, held, sent, None)
    w_wait(NC - 1)
    end([NC - 1], early)
    far(NC - 2)
    far(NC - 1)
    end([NC - 2, NC - 1], late)
    lax.fori_loop(held, NC, sent, None)
    for i in range(4):
        wo_start(i)

    e = HEAD**-0.5 * LOG2E
    ones = jnp.ones((8, R), BF)

    tall = HEAD + 8

    def attend(b, at_q, first, size):
        parts = [(q, q // HEAD * 2 * HEAD, min(HEAD, size - q)) for q in range(0, size, HEAD)]

        def mix(h):
            return jnp.concatenate([acc[h, at : at + tall, :w] for _, at, w in parts], axis=1)

        for h in range(H):
            top_s[h : h + 1, :size] = jnp.full((1, size), NEG, F32)
            for _, at, w in parts:
                acc[h, at : at + tall, :w] = jnp.zeros((tall, w), F32)

        def block(j, masked):
            keys = rows(swap(lax.rem(j - me + n_tp, n_tp)))
            scores = [_dot(xg[H + h, keys, :], xg[h, at_q, :], 1, 1) for h in range(H)]
            weights, keeps = [], []
            for h, s in enumerate(scores):
                if masked:
                    ok = lax.broadcasted_iota(jnp.int32, (R, size), 1) + first >= lax.broadcasted_iota(jnp.int32, (R, size), 0)
                    s = jnp.where(ok, s, HIDDEN)
                old = top_s[h : h + 1, :size]
                top = jnp.maximum(old, s.max(axis=0, keepdims=True))
                top_s[h : h + 1, :size] = top
                weights.append(jnp.exp2((s - top) * e).astype(BF))
                keeps.append(jnp.exp2((old - top) * e))
            for h, (p, keep) in enumerate(zip(weights, keeps)):
                values = jnp.concatenate([xg[2 * H + h, keys, :].T, ones], axis=0)
                new = mix(h) * keep + _dot(values, p, 1, 0)
                for q, at, w in parts:
                    acc[h, at : at + tall, :w] = new[:, q : q + w]

        lax.fori_loop(0, b, lambda j, _: block(j, False), None)
        block(b, True)
        for h in range(H):
            got = mix(h)
            xg[3 * H + h, at_q, :] = (got[:HEAD] * (1 / got[HEAD : HEAD + 1])).T.astype(BF)

    half = KC // 2

    def opp_tile(s, n, first, size):
        wo_wait(s)
        for at in (0, half):
            r = jnp.dot(seen(rows(OPP, first, size)), wo_cols(s, at, half), preferred_element_type=F32)
            s_opp[n, pl.ds(first, size), at : at + half] = r.astype(BF)

    def opp_half(side, _):
        first = pl.multiple_of(side * R2, R2)
        attend(lax.rem(me + 2, n_tp), rows(OPP, first, R2), first, R2)

        def tile(n, _):
            s = side * FIRST + n
            opp_tile(s, n, first, R2)
            for way in range(2):
                rs(2 * side + way, n).start()
            wo_start(s + 4)

        lax.fori_loop(0, FIRST, tile, None)

    def opp_whole(n, _):
        opp_tile(n + FIRST, n, 0, R)
        for kind in range(4):
            rs(kind, n).start()
        wo_start(n + FIRST + 4)

    lax.fori_loop(0, 2, opp_half, None)
    lax.fori_loop(FIRST, NC, opp_whole, None)

    def others(i, _):
        place = lax.rem(i + 1, 3)
        attend(lax.rem(me + swap(place), n_tp), rows(place), 0, R)

    lax.fori_loop(0, 3, others, None)

    for k, other in enumerate((left, right)):
        pl.semaphore_signal(free_sem.at[k], inc=1, device_id={"tp": other}, device_id_type=MESH)

    for k in range(2):
        pl.semaphore_wait(free_sem.at[k], 1)

    def send_full(n):
        s = n + FIRST + NC
        wo_wait(s)
        for kind in range(4):
            rs(kind, n).wait_recv()

        @pl.when(n >= SLOTS)
        def _():
            rs(4, n - SLOTS).wait_send()
            rs(5, n - SLOTS).wait_send()

        slot = lax.rem(n, SLOTS)
        lhs = seen(early)
        for at in (0, half):
            r = jnp.dot(lhs, wo_cols(s, at, half), preferred_element_type=F32)
            for j in range(half // HEAD):
                own, to_right, to_left = (r[b * R : (b + 1) * R, j * HEAD : (j + 1) * HEAD] for b in range(3))
                here, first = slice(at + j * HEAD, at + (j + 1) * HEAD), (at // HEAD + j) * R
                for q in range(4):
                    quarter, came = slice(q * R4, (q + 1) * R4), r_half[q % 2, n, q // 2 * R4 : (q // 2 + 1) * R4, here].astype(F32)
                    for way, t in enumerate((to_right[quarter], to_left[quarter])):
                        s_full[way, slot, first + q * R4 : first + (q + 1) * R4, :] = (t + came if q % 2 == way else t).astype(BF)
                acc[n, rows(at // HEAD + j), :] = own
        rs(4, n).start()
        rs(5, n).start()

        @pl.when(n + 4 < NC)
        def _():
            wo_start(s + 4)

    def finish(n):
        rs(4, n).wait_recv()
        rs(5, n).wait_recv()
        for j in range(UC):
            here = rows(j)
            total = acc[n, here, :] + xg[n, here, :].astype(F32) + xg[H + n, here, :].astype(F32)
            y_ref[:, cols(n * UC + j)] = (y_ref[:, cols(n * UC + j)].astype(F32) + total).astype(BF)

    def both(n, _):
        @pl.when(n < NC)
        def _():
            send_full(n)

        @pl.when(n >= SLOTS)
        def _():
            finish(n - SLOTS)

    lax.fori_loop(0, NC + SLOTS, both, None)

    def close(n, _):
        for kind in range(4):
            rs(kind, n).wait_send()

        @pl.when(n >= NC - SLOTS)
        def _():
            rs(4, n).wait_send()
            rs(5, n).wait_send()

    lax.fori_loop(0, NC, close, None)


PARTS = 4


def _move(a_ref, b_ref, sem):
    size = a_ref.shape[0] // PARTS
    copies = [pltpu.make_async_copy(a_ref.at[i * size : (i + 1) * size], b_ref.at[i * size : (i + 1) * size], sem.at[i]) for i in range(PARTS)]
    for c in copies:
        c.start()
    for c in copies:
        c.wait()


def moved(a):
    return pl.pallas_call(
        _move,
        out_shape=jax.ShapeDtypeStruct(a.shape, a.dtype),
        in_specs=[pl.BlockSpec(memory_space=pltpu.VMEM)],
        out_specs=pl.BlockSpec(memory_space=pl.ANY),
        scratch_shapes=[pltpu.SemaphoreType.DMA((PARTS,))],
        compiler_params=pltpu.CompilerParams(vmem_limit_bytes=8 * 2**20),
        cost_estimate=pl.CostEstimate(flops=1, bytes_accessed=4 * a.size, transcendentals=0),
    )(a)


def layer(x, gain, wq, wk, wv, wo, n_tp):
    R, D = x.shape
    HK = wo.shape[0]
    H = HK // HEAD
    T, U, NC = n_tp * R, D // HEAD, D // KC
    half = HEAD // 2
    freq = np.tile(np.float32(THETA) ** (-np.arange(half, dtype=np.float32) / np.float32(half)), 2)[None]
    any_ = pl.BlockSpec(memory_space=pl.ANY)
    dma = pltpu.SemaphoreType.DMA
    y = pl.pallas_call(
        _kernel,
        out_shape=pltpu.VMEM((R, D), BF),
        in_specs=[any_] * 7,
        out_specs=pl.BlockSpec(memory_space=pltpu.VMEM),
        scratch_shapes=[
            pltpu.VMEM((U, T, HEAD), BF),
            pltpu.VMEM((3 * H, T, HEAD), F32),
            pltpu.VMEM((2, KC, 3 * HK), BF),
            pltpu.VMEM((T, HEAD), F32),
            pltpu.VMEM((T, HEAD), F32),
            pltpu.VMEM((H, R), F32),
            pltpu.VMEM((D,), BF),
            pltpu.VMEM((1, HEAD), F32),
            pltpu.VMEM((NC, R, KC), BF),
            pltpu.VMEM((2, SLOTS, UC * R, HEAD), BF),
            pltpu.VMEM((2, NC, R // 2, KC), BF),
            dma((4, NC)), dma((4, NC)), dma((6, NC)), dma((6, NC)),
            dma((2, 3)), dma((4, -(-HK // KC))), dma((R // 32,)), dma((2,)), pltpu.SemaphoreType.REGULAR((2,)),
        ],
        compiler_params=pltpu.CompilerParams(collective_id=0, has_side_effects=True, vmem_limit_bytes=63000000),
        cost_estimate=pl.CostEstimate(flops=8 * T * D * HK, bytes_accessed=8 * D * HK, transcendentals=H * T * T),
    )(x, gain, jnp.asarray(freq), wq, wk, wv, wo)
    return moved(y)


def solution(mesh):
    tokens, columns = P(("dp", "tp"), None), P(None, "tp")
    return jax.shard_map(
        functools.partial(layer, n_tp=mesh.shape["tp"]),
        mesh=mesh,
        in_specs=(tokens, P(None), columns, columns, columns, P("tp", None)),
        out_specs=tokens,
        check_vma=False,
    )
```
